128 devices in a mesh: rep: 2 (over core), dp: 64 (over x, y, z).
Axes of the slice: x: 4, y: 4, z: 4, core: 2. Of those that a mesh axis runs over, the one named last changes fastest.
Arguments:
- x: bfloat16 [128, 2048, 512], P(('rep', 'dp')), parts along dimension 0
- dy: bfloat16 [128, 2048, 512], P(('rep', 'dp')), parts along dimension 0
- w_gate: bfloat16 [2, 512, 4096], replicated
- w_up: bfloat16 [2, 512, 4096], replicated
- w_down: bfloat16 [2, 4096, 512], replicated
- m_w_gate: float32 [2, 512, 4096], replicated
- m_w_up: float32 [2, 512, 4096], replicated
- m_w_down: float32 [2, 4096, 512], replicated
- v_w_gate: float32 [2, 512, 4096], replicated
- v_w_up: float32 [2, 512, 4096], replicated
- v_w_down: float32 [2, 4096, 512], replicated
Outputs:
- output 1: bfloat16 [4, 512, 4096], P('rep'), parts along dimension 0
- output 2: bfloat16 [4, 512, 4096], P('rep'), parts along dimension 0
- output 3: bfloat16 [4, 4096, 512], P('rep'), parts along dimension 0
- output 4: float32 [4, 512, 4096], P('rep'), parts along dimension 0
- output 5: float32 [4, 512, 4096], P('rep'), parts along dimension 0
- output 6: float32 [4, 4096, 512], P('rep'), parts along dimension 0
- output 7: float32 [4, 512, 4096], P('rep'), parts along dimension 0
- output 8: float32 [4, 512, 4096], P('rep'), parts along dimension 0
- output 9: float32 [4, 4096, 512], P('rep'), parts along dimension 0
There are 2 independent parts. The reference program is written for one: setup_inputs(seed, part) draws one part's arguments, and reference() takes and returns one part's arrays. A program takes and returns all parts, laid end to end along the dimension named above; an argument that names none is the same for every part.
All inputs are finite; a program needn't handle non-finite values.
Results may differ from the reference program's by a relative error of at most 0.022.
Values are sent between devices in bfloat16 or wider.
A program may use at most 1.5 GiB of HBM per device.

```python
import jax
import jax.numpy as jnp
from jax import lax

SEQUENCES = 64
TOKENS = 2048
D = 512
FF = 4096
LAYERS = 2
NAMES = ("w_gate", "w_up", "w_down")
SHAPES = {"w_gate": (LAYERS, D, FF), "w_up": (LAYERS, D, FF), "w_down": (LAYERS, FF, D)}


def bump(key, n, height):
    away = (jnp.arange(n, dtype=jnp.int32) - jax.random.randint(key, (), 0, n, jnp.int32)) % n
    return jnp.where(away < n // 8, height, 1.0)


def together(key, own, strength):
    shared = jax.random.normal(key, own.shape[1:], jnp.float32)
    return (own + strength * shared) * lax.rsqrt(1 + strength * strength)


def setup_inputs(seed: int = 0, part: int = 0) -> dict:
    kx, kdy, ka, kb, kz, kf, kh, kl, *keys = jax.random.split(jax.random.key(seed), 8 + 3 * len(NAMES))
    kx, kdy, ka, kb = (jax.random.fold_in(k, part) for k in (kx, kdy, ka, kb))
    kw, km, kv = (keys[i::3] for i in range(3))
    shape = (SEQUENCES, TOKENS, D)
    much_x, much_dy = jax.random.uniform(kz, (2,), jnp.float32, 0.0, 1.0)
    loud = 2.0 ** jax.random.uniform(jax.random.fold_in(kz, 1), (), jnp.float32, -1.0, 2.0)
    layers = 2.0 ** jax.random.uniform(kl, (LAYERS, 1, 1), jnp.float32, -1.0, 1.0)
    x = together(ka, jax.random.normal(kx, shape, jnp.float32), much_x) * bump(kf, D, 4.0)
    dy = together(kb, jax.random.normal(kdy, shape, jnp.float32), much_dy)
    drawn = {"x": x.astype(jnp.bfloat16), "dy": (loud * dy * (SEQUENCES * TOKENS) ** -0.5).astype(jnp.bfloat16)}
    for key, name in zip(kw, NAMES, strict=True):
        w = jax.random.normal(key, SHAPES[name], jnp.float32) * SHAPES[name][1] ** -0.5
        drawn[name] = (w * {"w_gate": 1.0, "w_up": bump(kh, FF, 4.0), "w_down": layers}[name]).astype(jnp.bfloat16)
    for key, name in zip(km, NAMES, strict=True):
        drawn[f"m_{name}"] = 0.1 * jax.random.normal(key, SHAPES[name], jnp.float32)
    for key, name in zip(kv, NAMES, strict=True):
        drawn[f"v_{name}"] = jax.random.uniform(key, SHAPES[name], jnp.float32, 0.005, 0.015)
    return drawn


def matmul(a, w):
    return jnp.dot(a, w, preferred_element_type=jnp.float32).astype(jnp.bfloat16)


def normed(h):
    wide = h.astype(jnp.float32)
    scale = lax.rsqrt(jnp.mean(wide**2, -1, keepdims=True) + 1e-6)
    return (wide * scale).astype(jnp.bfloat16)


def layer(h, w):
    a = normed(h)
    gate = jnp.dot(a, w["w_gate"], preferred_element_type=jnp.float32)
    up = jnp.dot(a, w["w_up"], preferred_element_type=jnp.float32)
    return h + matmul((jax.nn.silu(gate) * up).astype(jnp.bfloat16), w["w_down"])


def adamw(w, m, v, g):
    m = 0.9 * m + 0.1 * g
    v = 0.95 * v + 0.05 * g * g
    step = m * lax.rsqrt(v + 1e-8) + 0.1 * w
    return (w - 0.02 * step).astype(jnp.bfloat16), m, v


def clipped(gradients, sum_of_squares, count):
    factor = jnp.minimum(1.0, 0.5 * lax.rsqrt(sum_of_squares / count + 1e-30))
    return [g * factor for g in gradients]


def stack(weights, h):
    return lax.scan(lambda h, w: (layer(h, w), None), h, weights)[0]


def reference(x, dy, w_gate, w_up, w_down, m_w_gate, m_w_up, m_w_down, v_w_gate, v_w_up, v_w_down):
    weights = dict(zip(NAMES, (w_gate, w_up, w_down), strict=True))

    def take(so_far, sequence):
        h, by_y = sequence
        _, back = jax.vjp(lambda w: stack(w, h), weights)
        return jax.tree.map(lambda total, term: total + term.astype(jnp.float32), so_far, back(by_y)[0]), None

    none_yet = {name: jnp.zeros(w.shape, jnp.float32) for name, w in weights.items()}
    by_weights, _ = lax.scan(take, none_yet, (x, dy))
    gradients = [by_weights[name].astype(jnp.bfloat16).astype(jnp.float32) for name in NAMES]
    gradients = clipped(gradients, sum(jnp.sum(g * g) for g in gradients), sum(g.size for g in gradients))
    new = [
        adamw(w.astype(jnp.float32), m, v, g)
        for w, m, v, g in zip((w_gate, w_up, w_down), (m_w_gate, m_w_up, m_w_down), (v_w_gate, v_w_up, v_w_down), gradients, strict=True)
    ]
    return tuple(one[which] for which in range(3) for one in new)
```

```python
import functools

import jax
import jax.numpy as jnp
from jax import lax
from jax.experimental import pallas as pl
from jax.experimental.pallas import tpu as pltpu
from jax.sharding import PartitionSpec as P

NAMES = ("w_gate", "w_up", "w_down")
T, D, FF, LAYERS = 2048, 512, 4096, 2
CH = 512
PER = FF // CH
N = PER * LAYERS
TILE = 512
PHASES = T // TILE
COLOURS = 6
ROWS = 1024
AT = [3 + o for o in (0, 2, 4, 5, 6, 7, 8, 9, 10, 11, 12, 14, 16, 17)]
ACCS, GATHERS = 3, 4
VMEM_LIMIT = 66_000_000

dot = functools.partial(lax.dot_general, preferred_element_type=jnp.float32)
NN = (((1,), (0,)), ((), ()))
NT = (((1,), (1,)), ((), ()))
TN = (((0,), (0,)), ((), ()))


def scale_of(wide):
    return lax.rsqrt(jnp.mean(wide * wide, -1, keepdims=True) + 1e-6)


def normed(h):
    wide = h.astype(jnp.float32)
    return (wide * scale_of(wide)).astype(jnp.bfloat16)


def forward_kernel(x_ref, wg_ref, wu_ref, wd_ref, h_ref, a_ref):
    x = x_ref[...]
    a = normed(x)
    a_ref[1] = a
    y = jnp.zeros(x.shape, jnp.float32)
    for c in range(FF // CH):
        at = pl.ds(c * CH, CH)
        gate = dot(a, wg_ref[0, :, at], NN)
        up = dot(a, wu_ref[0, :, at], NN)
        p = (gate * (1 / (1 + jnp.exp(-gate))) * up).astype(jnp.bfloat16)
        y += dot(p, wd_ref[0, at, :], NN)
    h = (x.astype(jnp.float32) + y.astype(jnp.bfloat16).astype(jnp.float32)).astype(jnp.bfloat16)
    h_ref[...] = h
    a_ref[0] = normed(h)


def forward(x, wg, wu, wd):
    tile = 256
    whole = lambda s: pl.BlockSpec(s, lambda i: (0, 0, 0), pipeline_mode=pl.Buffered(1))
    return pl.pallas_call(
        forward_kernel,
        grid=(T // tile,),
        in_specs=[pl.BlockSpec((tile, D), lambda i: (i, 0)), whole((1, D, FF)), whole((1, D, FF)), whole((1, FF, D))],
        out_specs=[pl.BlockSpec((tile, D), lambda i: (i, 0)), pl.BlockSpec((2, tile, D), lambda i: (0, i, 0))],
        out_shape=[jax.ShapeDtypeStruct((T, D), jnp.bfloat16), jax.ShapeDtypeStruct((2, T, D), jnp.bfloat16)],
        compiler_params=pltpu.CompilerParams(vmem_limit_bytes=VMEM_LIMIT),
    )(x, wg, wu, wd)


def place(stage):
    return ROWS - (ROWS >> stage)


def backward_kernel(
    a_ref, h_ref, dy_ref, wg_ref, wu_ref, wd_ref, gg_ref, gu_ref, gd_ref, squares_ref,
    ct, dag, dau, w, acc, outgoing, incoming, gathered, w_sem, sent_sem, got_sem, write_sem,
):
    rep, me = lax.axis_index("rep"), lax.axis_index("dp")
    at = [me // 16, (me // 4) % 4, me % 4]
    step = [16, 4, 1]
    side, partner = [], []
    for kind in range(2):
        for p, s in zip(at, step):
            other = p + 1 - 2 * (p % 2) if kind == 0 else 3 - p
            side.append(((p + 1) // 2) % 2 if kind == 0 else p // 2)
            partner.append(me + (other - p) * s)
    start = []
    for k in range(COLOURS):
        rows = [0]
        for s in range(6):
            rows.append(rows[-1] + side[(k + s) % 6] * (ROWS >> (s + 1)))
        start.append(rows)

    barrier = pltpu.get_barrier_semaphore()
    for other in partner:
        pl.semaphore_signal(barrier, inc=1, device_id=(rep, other), device_id_type=pl.DeviceIdType.MESH)
    pl.semaphore_wait(barrier, 6)

    squares_ref[...] = jnp.zeros_like(squares_ref)
    ct[0] = dy_ref[...]

    def weights(i):
        layer, at = LAYERS - 1 - i // PER, pl.ds(pl.multiple_of((i % PER) * CH, CH), CH)
        slot = i % 2
        return [
            pltpu.make_async_copy(wg_ref.at[layer, :, at], w.at[slot, 0], w_sem.at[slot, 0]),
            pltpu.make_async_copy(wu_ref.at[layer, :, at], w.at[slot, 1], w_sem.at[slot, 1]),
            pltpu.make_async_copy(wd_ref.at[layer, at, :], w.at[slot, 2], w_sem.at[slot, 2]),
        ]

    def rows_of(start, size):
        return pl.ds(pl.multiple_of(start, 16), size)

    def exchange(c, stage, k):
        even = c % 2
        if stage < 6:
            size, link = ROWS >> (stage + 1), (k + stage) % 6
            part = pl.ds(place(stage), size)
            source, target = outgoing.at[k, part], incoming.at[even, k, part]
        else:
            s = 11 - stage
            size, link = ROWS >> (s + 1), (k + s) % 6
            source = target = gathered.at[c % GATHERS, k, rows_of(start[k][s + 1], size)]
        return pltpu.make_async_remote_copy(
            src_ref=source,
            dst_ref=target,
            send_sem=sent_sem.at[stage, k],
            recv_sem=got_sem.at[even, stage, k],
            device_id=(rep, partner[link]),
            device_id_type=pl.DeviceIdType.MESH,
        )

    def writes(c):
        layer, first = LAYERS - 1 - c // PER, (c % PER) * CH
        slot, copies = c % GATHERS, []
        for k in range(COLOURS):
            matrix, half = k // 2, (k % 2) * 256
            for b in range(4):
                source = gathered.at[slot, k, pl.ds(b * 256, 256)]
                if matrix < 2:
                    to = (gg_ref, gu_ref)[matrix].at[layer, pl.ds(half, 256), pl.ds(pl.multiple_of(first + b * 128, 128), 128)]
                else:
                    to = gd_ref.at[layer, pl.ds(pl.multiple_of(first + half, 256), 256), pl.ds(b * 128, 128)]
                copies.append(pltpu.make_async_copy(source, to, write_sem.at[k, b]))
        return copies

    def stage_of(stage, c):
        slot, even, gather = c % ACCS, c % 2, c % GATHERS
        if stage == 13:
            for copy in writes(c):
                copy.wait()
            return
        for k in range(COLOURS):
            if stage > 0:
                exchange(c, stage - 1, k).wait()
            if stage < 6:
                size = ROWS >> (stage + 1)
                mine, theirs = side[(k + stage) % 6] * size, (1 - side[(k + stage) % 6]) * size
                goes = acc[slot, k, rows_of(start[k][stage] + theirs, size)]
                if stage > 0:
                    base = place(stage - 1)
                    goes += incoming[even, k, rows_of(base + theirs, size)].astype(jnp.float32)
                    stays = rows_of(start[k][stage] + mine, size)
                    acc[slot, k, stays] += incoming[even, k, rows_of(base + mine, size)].astype(jnp.float32)
                outgoing[k, pl.ds(place(stage), size)] = goes.astype(jnp.bfloat16)
            elif stage == 6:
                rows = rows_of(start[k][6], 16)
                total = acc[slot, k, rows] + incoming[even, k, pl.ds(place(5), 16)].astype(jnp.float32)
                gathered[gather, k, rows] = total.astype(jnp.bfloat16)
            if stage < 12:
                exchange(c, stage, k).start()
        if stage == 12:
            for copy in writes(c):
                copy.start()
            for k in range(COLOURS):
                g = gathered[gather, k].astype(jnp.float32)
                squares_ref[...] += jnp.sum((g * g).reshape(ROWS // 8, 8, 128), axis=0)

    def tile_of(i, phase):
        turn, slot, a_slot = i // PER, i % 2, i % ACCS
        tokens = pl.ds(phase * TILE, TILE)
        a, by = a_ref[turn, tokens, :], ct[turn, tokens, :]
        gate = dot(a, w[slot, 0], NN)
        up = dot(a, w[slot, 1], NN)
        by_p = dot(by, w[slot, 2], NT).astype(jnp.bfloat16).astype(jnp.float32)
        sigmoid = 1 / (1 + jnp.exp(-gate))
        silu = gate * sigmoid
        p = (silu * up).astype(jnp.bfloat16)
        by_up = (by_p * silu).astype(jnp.bfloat16)
        by_gate = (by_p * up * (sigmoid * (1 + gate * (1 - sigmoid)))).astype(jnp.bfloat16)
        for matrix, (l, r) in enumerate(((a, by_gate), (a, by_up), (p, by))):
            g = dot(l, r, TN)
            for half in range(2):
                for b in range(4):
                    part = g[half * 256 : half * 256 + 256, b * 128 : b * 128 + 128]
                    if phase == 0:
                        acc[a_slot, 2 * matrix + half, pl.ds(b * 256, 256)] = part
                    else:
                        acc[a_slot, 2 * matrix + half, pl.ds(b * 256, 256)] += part

        @pl.when(i < PER)
        def _():
            dag[tokens, :] += dot(by_gate, w[slot, 0], NT)
            dau[tokens, :] += dot(by_up, w[slot, 1], NT)

    def next_layer():
        def body(t, _):
            tokens = pl.ds(pl.multiple_of(t * 256, 256), 256)
            d = (dag[tokens, :].astype(jnp.bfloat16).astype(jnp.float32) + dau[tokens, :].astype(jnp.bfloat16).astype(jnp.float32)).astype(jnp.bfloat16)
            d, wide = d.astype(jnp.float32), h_ref[tokens, :].astype(jnp.float32)
            s = scale_of(wide)
            by = d * s - wide * (s * s * s * jnp.sum(d * wide, -1, keepdims=True) * (1 / D))
            ct[1, tokens, :] = (ct[0, tokens, :].astype(jnp.float32) + by.astype(jnp.bfloat16).astype(jnp.float32)).astype(jnp.bfloat16)
            return 0

        lax.fori_loop(0, T // 256, body, 0)

    def clear(t, _):
        tokens = pl.ds(pl.multiple_of(t * 256, 256), 256)
        dag[tokens, :] = jnp.zeros((256, D), jnp.float32)
        dau[tokens, :] = jnp.zeros((256, D), jnp.float32)
        return 0

    for copy in weights(0):
        copy.start()
    lax.fori_loop(0, T // 256, clear, 0)

    def body(i, _):
        @pl.when(i < N)
        def _():
            for copy in weights(i):
                copy.wait()

        @pl.when(i + 1 < N)
        def _():
            for copy in weights(i + 1):
                copy.start()

        pl.when(i == PER)(next_layer)

        for phase in range(PHASES):
            pl.when(i < N)(functools.partial(tile_of, i, phase))
            for stage in reversed(range(len(AT))):
                if AT[stage] % PHASES == phase:
                    c = i - AT[stage] // PHASES
                    pl.when((c >= 0) & (c < N))(functools.partial(stage_of, stage, c))
        return 0

    lax.fori_loop(0, N + AT[-1] // PHASES, body, 0)


def backward(a, h, dy, wg, wu, wd):
    vmem, anywhere = pl.BlockSpec(memory_space=pltpu.VMEM), pl.BlockSpec(memory_space=pl.ANY)
    dma = pltpu.SemaphoreType.DMA
    return pl.pallas_call(
        backward_kernel,
        in_specs=[vmem] * 3 + [anywhere] * 3,
        out_specs=[anywhere] * 3 + [vmem],
        out_shape=[
            jax.ShapeDtypeStruct((LAYERS, D, FF), jnp.bfloat16),
            jax.ShapeDtypeStruct((LAYERS, D, FF), jnp.bfloat16),
            jax.ShapeDtypeStruct((LAYERS, FF, D), jnp.bfloat16),
            jax.ShapeDtypeStruct((8, 128), jnp.float32),
        ],
        scratch_shapes=[
            pltpu.VMEM((2, T, D), jnp.bfloat16),
            pltpu.VMEM((T, D), jnp.float32),
            pltpu.VMEM((T, D), jnp.float32),
            pltpu.VMEM((2, 3, D, CH), jnp.bfloat16),
            pltpu.VMEM((ACCS, COLOURS, ROWS, 128), jnp.float32),
            pltpu.VMEM((COLOURS, ROWS, 128), jnp.bfloat16),
            pltpu.VMEM((2, COLOURS, ROWS, 128), jnp.bfloat16),
            pltpu.VMEM((GATHERS, COLOURS, ROWS, 128), jnp.bfloat16),
            dma((2, 3)),
            dma((12, COLOURS)),
            dma((2, 12, COLOURS)),
            dma((COLOURS, 4)),
        ],
        compiler_params=pltpu.CompilerParams(collective_id=0, has_side_effects=True, vmem_limit_bytes=VMEM_LIMIT),
    )(a, h, dy, wg, wu, wd)


def adamw(w, m, v, g):
    m = 0.9 * m + 0.1 * g
    v = 0.95 * v + 0.05 * g * g
    step = m * lax.rsqrt(v + 1e-8) + 0.1 * w
    return (w - 0.02 * step).astype(jnp.bfloat16), m, v


def solution(mesh):
    def step(x, dy, *arrays):
        weights, m, v = (arrays[i : i + 3] for i in (0, 3, 6))
        h, a = forward(x[0], *weights)
        *gradients, squares = backward(a, h, dy[0], *weights)
        count = sum(g.size for g in gradients)
        factor = jnp.minimum(1.0, 0.5 * lax.rsqrt(jnp.sum(squares) / count + 1e-30))
        new = [adamw(w.astype(jnp.float32), m, v, g.astype(jnp.float32) * factor) for w, m, v, g in zip(weights, m, v, gradients, strict=True)]
        return tuple(one[which] for which in range(3) for one in new)

    return jax.shard_map(
        step,
        mesh=mesh,
        in_specs=(P(("rep", "dp"), None, None),) * 2 + (P(None, None, None),) * 9,
        out_specs=(P("rep", None, None),) * 9,
        check_vma=False,
    )
```

```python
import functools

import jax
import jax.numpy as jnp
from jax import lax
from jax.experimental import pallas as pl
from jax.experimental.pallas import tpu as pltpu
from jax.sharding import PartitionSpec as P

NAMES = ("w_gate", "w_up", "w_down")
T, D, FF, LAYERS = 2048, 512, 4096, 2
CH = 512
PER = FF // CH
N = PER * LAYERS
TILE = 512
PHASES = T // TILE
COLOURS = 6
ROWS = 1024
AT = [3 + o for o in (0, 4, 7, 9, 11, 13, 15, 17, 19, 21, 23, 26, 30, 31)]
ACCS, GATHERS = 5, 5
VMEM_LIMIT = 66_000_000

dot = functools.partial(lax.dot_general, preferred_element_type=jnp.float32)
NN = (((1,), (0,)), ((), ()))
NT = (((1,), (1,)), ((), ()))
TN = (((0,), (0,)), ((), ()))


def scale_of(wide):
    return lax.rsqrt(jnp.mean(wide * wide, -1, keepdims=True) + 1e-6)


def normed(h):
    wide = h.astype(jnp.float32)
    return (wide * scale_of(wide)).astype(jnp.bfloat16)


def place(stage):
    return ROWS - (ROWS >> stage)


def kernel(
    x_ref, dy_ref, wg_ref, wu_ref, wd_ref, gg_ref, gu_ref, gd_ref, squares_ref,
    h_ref, a_ref, ct, dag, dau, w, acc, outgoing, incoming, gathered, in_sem, w_sem, sent_sem, got_sem, write_sem,
):
    rep, me = lax.axis_index("rep"), lax.axis_index("dp")
    at = [me // 16, (me // 4) % 4, me % 4]
    step = [16, 4, 1]
    side, partner = [], []
    for kind in range(2):
        for p, s in zip(at, step):
            other = p + 1 - 2 * (p % 2) if kind == 0 else 3 - p
            side.append(((p + 1) // 2) % 2 if kind == 0 else p // 2)
            partner.append(me + (other - p) * s)
    start = []
    for k in range(COLOURS):
        rows = [0]
        for s in range(6):
            rows.append(rows[-1] + side[(k + s) % 6] * (ROWS >> (s + 1)))
        start.append(rows)

    barrier = pltpu.get_barrier_semaphore()
    for other in partner:
        pl.semaphore_signal(barrier, inc=1, device_id=(rep, other), device_id_type=pl.DeviceIdType.MESH)
    squares_ref[...] = jnp.zeros_like(squares_ref)

    def weights(i):
        layer, at = ((i + PER) // PER) % 2, pl.ds(pl.multiple_of(((i + PER) % PER) * CH, CH), CH)
        slot = (i + PER) % 2
        return [
            pltpu.make_async_copy(wg_ref.at[layer, :, at], w.at[slot, 0], w_sem.at[slot, 0]),
            pltpu.make_async_copy(wu_ref.at[layer, :, at], w.at[slot, 1], w_sem.at[slot, 1]),
            pltpu.make_async_copy(wd_ref.at[layer, at, :], w.at[slot, 2], w_sem.at[slot, 2]),
        ]

    def rows_of(start, size):
        return pl.ds(pl.multiple_of(start, 16), size)

    def exchange(c, stage, k):
        even = c % 2
        if stage < 6:
            size, link = ROWS >> (stage + 1), (k + stage) % 6
            part = pl.ds(place(stage), size)
            source, target = outgoing.at[k, part], incoming.at[even, k, part]
        else:
            s = 11 - stage
            size, link = ROWS >> (s + 1), (k + s) % 6
            source = target = gathered.at[c % GATHERS, k, rows_of(start[k][s + 1], size)]
        return pltpu.make_async_remote_copy(
            src_ref=source,
            dst_ref=target,
            send_sem=sent_sem.at[stage, k],
            recv_sem=got_sem.at[even, stage, k],
            device_id=(rep, partner[link]),
            device_id_type=pl.DeviceIdType.MESH,
        )

    def writes(c):
        layer, first = LAYERS - 1 - c // PER, (c % PER) * CH
        slot, copies = c % GATHERS, []
        for k in range(COLOURS):
            matrix, half = k // 2, (k % 2) * 256
            for b in range(4):
                source = gathered.at[slot, k, pl.ds(b * 256, 256)]
                if matrix < 2:
                    to = (gg_ref, gu_ref)[matrix].at[layer, pl.ds(half, 256), pl.ds(pl.multiple_of(first + b * 128, 128), 128)]
                else:
                    to = gd_ref.at[layer, pl.ds(pl.multiple_of(first + half, 256), 256), pl.ds(b * 128, 128)]
                copies.append(pltpu.make_async_copy(source, to, write_sem.at[k, b]))
        return copies

    def stage_of(stage, c):
        slot, even, gather = c % ACCS, c % 2, c % GATHERS
        if stage == 13:
            for copy in writes(c):
                copy.wait()
            return
        for k in range(COLOURS):
            if stage > 0:
                exchange(c, stage - 1, k).wait()
            if stage < 6:
                size = ROWS >> (stage + 1)
                mine, theirs = side[(k + stage) % 6] * size, (1 - side[(k + stage) % 6]) * size
                goes = acc[slot, k, rows_of(start[k][stage] + theirs, size)]
                if stage > 0:
                    base = place(stage - 1)
                    goes += incoming[even, k, rows_of(base + theirs, size)].astype(jnp.float32)
                    stays = rows_of(start[k][stage] + mine, size)
                    acc[slot, k, stays] += incoming[even, k, rows_of(base + mine, size)].astype(jnp.float32)
                outgoing[k, pl.ds(place(stage), size)] = goes.astype(jnp.bfloat16)
            elif stage == 6:
                rows = rows_of(start[k][6], 16)
                total = acc[slot, k, rows] + incoming[even, k, pl.ds(place(5), 16)].astype(jnp.float32)
                gathered[gather, k, rows] = total.astype(jnp.bfloat16)
            if stage < 12:
                exchange(c, stage, k).start()
        if stage == 12:
            for copy in writes(c):
                copy.start()
            for k in range(COLOURS):
                g = gathered[gather, k].astype(jnp.float32)
                squares_ref[...] += jnp.sum((g * g).reshape(ROWS // 8, 8, 128), axis=0)

    def tile_of(i, phase):
        turn, slot, a_slot = i // PER, i % 2, i % ACCS
        tokens = pl.ds(phase * TILE, TILE)
        a, by = a_ref[turn, tokens, :], ct[turn, tokens, :]
        gate = dot(a, w[slot, 0], NN)
        up = dot(a, w[slot, 1], NN)
        by_p = dot(by, w[slot, 2], NT).astype(jnp.bfloat16).astype(jnp.float32)
        sigmoid = 1 / (1 + jnp.exp(-gate))
        silu = gate * sigmoid
        p = (silu * up).astype(jnp.bfloat16)
        by_up = (by_p * silu).astype(jnp.bfloat16)
        by_gate = (by_p * up * (sigmoid * (1 + gate * (1 - sigmoid)))).astype(jnp.bfloat16)
        for matrix, (l, r) in enumerate(((a, by_gate), (a, by_up), (p, by))):
            g = dot(l, r, TN)
            for half in range(2):
                for b in range(4):
                    part = g[half * 256 : half * 256 + 256, b * 128 : b * 128 + 128]
                    if phase == 0:
                        acc[a_slot, 2 * matrix + half, pl.ds(b * 256, 256)] = part
                    else:
                        acc[a_slot, 2 * matrix + half, pl.ds(b * 256, 256)] += part

        @pl.when(i < PER)
        def _():
            dag[tokens, :] += dot(by_gate, w[slot, 0], NT)
            dau[tokens, :] += dot(by_up, w[slot, 1], NT)

    def next_layer():
        def body(t, _):
            tokens = pl.ds(pl.multiple_of(t * 256, 256), 256)
            d = (dag[tokens, :].astype(jnp.bfloat16).astype(jnp.float32) + dau[tokens, :].astype(jnp.bfloat16).astype(jnp.float32)).astype(jnp.bfloat16)
            d, wide = d.astype(jnp.float32), h_ref[tokens, :].astype(jnp.float32)
            s = scale_of(wide)
            by = d * s - wide * (s * s * s * jnp.sum(d * wide, -1, keepdims=True) * (1 / D))
            ct[1, tokens, :] = (ct[0, tokens, :].astype(jnp.float32) + by.astype(jnp.bfloat16).astype(jnp.float32)).astype(jnp.bfloat16)
            return 0

        lax.fori_loop(0, T // 256, body, 0)

    def first(t, _):
        tokens = pl.ds(pl.multiple_of(t * 256, 256), 256)
        a_ref[1, tokens, :] = normed(h_ref[tokens, :])
        dag[tokens, :] = jnp.zeros((256, D), jnp.float32)
        return 0

    def forward(i, _):
        for copy in weights(i):
            copy.wait()
        for copy in weights(i + 1):
            copy.start()
        slot = (i + PER) % 2

        def tile(t, _):
            tokens = pl.ds(pl.multiple_of(t * TILE, TILE), TILE)
            a = a_ref[1, tokens, :]
            gate = dot(a, w[slot, 0], NN)
            up = dot(a, w[slot, 1], NN)
            p = (gate * (1 / (1 + jnp.exp(-gate))) * up).astype(jnp.bfloat16)
            dag[tokens, :] += dot(p, w[slot, 2], NN)
            return 0

        lax.fori_loop(0, PHASES, tile, 0)
        return 0

    def second(t, _):
        tokens = pl.ds(pl.multiple_of(t * 256, 256), 256)
        h = (h_ref[tokens, :].astype(jnp.float32) + dag[tokens, :].astype(jnp.bfloat16).astype(jnp.float32)).astype(jnp.bfloat16)
        h_ref[tokens, :] = h
        a_ref[0, tokens, :] = normed(h)
        dag[tokens, :] = jnp.zeros((256, D), jnp.float32)
        dau[tokens, :] = jnp.zeros((256, D), jnp.float32)
        return 0

    inputs = [pltpu.make_async_copy(x_ref, h_ref, in_sem.at[0]), pltpu.make_async_copy(dy_ref, ct.at[0], in_sem.at[1])]
    for copy in inputs + weights(-PER):
        copy.start()
    inputs[0].wait()
    lax.fori_loop(0, T // 256, first, 0)
    lax.fori_loop(-PER, 0, forward, 0)
    lax.fori_loop(0, T // 256, second, 0)
    inputs[1].wait()
    pl.semaphore_wait(barrier, 6)

    def body(i, _):
        @pl.when(i < N)
        def _():
            for copy in weights(i):
                copy.wait()

        @pl.when(i + 1 < N)
        def _():
            for copy in weights(i + 1):
                copy.start()

        pl.when(i == PER)(next_layer)

        for phase in range(PHASES):
            pl.when(i < N)(functools.partial(tile_of, i, phase))
            for stage in reversed(range(len(AT))):
                if AT[stage] % PHASES == phase:
                    c = i - AT[stage] // PHASES
                    pl.when((c >= 0) & (c < N))(functools.partial(stage_of, stage, c))
        return 0

    lax.fori_loop(0, N + AT[-1] // PHASES, body, 0)


def gradients_of(x, dy, wg, wu, wd):
    vmem, anywhere = pl.BlockSpec(memory_space=pltpu.VMEM), pl.BlockSpec(memory_space=pl.ANY)
    dma = pltpu.SemaphoreType.DMA
    return pl.pallas_call(
        kernel,
        in_specs=[anywhere] * 5,
        out_specs=[anywhere] * 3 + [vmem],
        out_shape=[
            jax.ShapeDtypeStruct((LAYERS, D, FF), jnp.bfloat16),
            jax.ShapeDtypeStruct((LAYERS, D, FF), jnp.bfloat16),
            jax.ShapeDtypeStruct((LAYERS, FF, D), jnp.bfloat16),
            jax.ShapeDtypeStruct((8, 128), jnp.float32),
        ],
        scratch_shapes=[
            pltpu.VMEM((T, D), jnp.bfloat16),
            pltpu.VMEM((2, T, D), jnp.bfloat16),
            pltpu.VMEM((2, T, D), jnp.bfloat16),
            pltpu.VMEM((T, D), jnp.float32),
            pltpu.VMEM((T, D), jnp.float32),
            pltpu.VMEM((2, 3, D, CH), jnp.bfloat16),
            pltpu.VMEM((ACCS, COLOURS, ROWS, 128), jnp.float32),
            pltpu.VMEM((COLOURS, ROWS, 128), jnp.bfloat16),
            pltpu.VMEM((2, COLOURS, ROWS, 128), jnp.bfloat16),
            pltpu.VMEM((GATHERS, COLOURS, ROWS, 128), jnp.bfloat16),
            dma((2,)),
            dma((2, 3)),
            dma((12, COLOURS)),
            dma((2, 12, COLOURS)),
            dma((COLOURS, 4)),
        ],
        compiler_params=pltpu.CompilerParams(collective_id=0, has_side_effects=True, vmem_limit_bytes=VMEM_LIMIT),
    )(x, dy, wg, wu, wd)


def adamw(w, m, v, g):
    m = 0.9 * m + 0.1 * g
    v = 0.95 * v + 0.05 * g * g
    step = m * lax.rsqrt(v + 1e-8) + 0.1 * w
    return (w - 0.02 * step).astype(jnp.bfloat16), m, v


def solution(mesh):
    def step(x, dy, *arrays):
        weights, m, v = (arrays[i : i + 3] for i in (0, 3, 6))
        *gradients, squares = gradients_of(x[0], dy[0], *weights)
        count = sum(g.size for g in gradients)
        factor = jnp.minimum(1.0, 0.5 * lax.rsqrt(jnp.sum(squares) / count + 1e-30))
        new = [adamw(w.astype(jnp.float32), m, v, g.astype(jnp.float32) * factor) for w, m, v, g in zip(weights, m, v, gradients, strict=True)]
        return tuple(one[which] for which in range(3) for one in new)

    return jax.shard_map(
        step,
        mesh=mesh,
        in_specs=(P(("rep", "dp"), None, None),) * 2 + (P(None, None, None),) * 9,
        out_specs=(P("rep", None, None),) * 9,
        check_vma=False,
    )
```

```python
import functools

import jax
import jax.numpy as jnp
from jax import lax
from jax.experimental import pallas as pl
from jax.experimental.pallas import tpu as pltpu
from jax.sharding import PartitionSpec as P

NAMES = ("w_gate", "w_up", "w_down")
T, D, FF, LAYERS = 2048, 512, 4096, 2
CH = 512
PER = FF // CH
N = PER * LAYERS
TILE = 512
PHASES = T // TILE
COLOURS = 6
ROWS = 1024
AT = [3 + o for o in (0, 4, 8, 11, 14, 16, 18, 20, 22, 24, 27, 31, 35, 36)]
ACCS, GATHERS = 6, 6
VMEM_LIMIT = 66_000_000

dot = functools.partial(lax.dot_general, preferred_element_type=jnp.float32)
NN = (((1,), (0,)), ((), ()))
NT = (((1,), (1,)), ((), ()))
TN = (((0,), (0,)), ((), ()))


def scale_of(wide):
    return lax.rsqrt(jnp.mean(wide * wide, -1, keepdims=True) + 1e-6)


def normed(h):
    wide = h.astype(jnp.float32)
    return (wide * scale_of(wide)).astype(jnp.bfloat16)


def place(stage):
    return ROWS - (ROWS >> stage)


def kernel(
    x_ref, dy_ref, wg_ref, wu_ref, wd_ref, gg_ref, gu_ref, gd_ref, squares_ref,
    h_ref, a_ref, ct, dag, dau, w, acc, outgoing, incoming, gathered, in_sem, w_sem, sent_sem, got_sem, write_sem,
):
    rep, me = lax.axis_index("rep"), lax.axis_index("dp")
    at = [me // 16, (me // 4) % 4, me % 4]
    step = [16, 4, 1]
    side, partner = [], []
    for kind in range(2):
        for p, s in zip(at, step):
            other = p + 1 - 2 * (p % 2) if kind == 0 else 3 - p
            side.append(((p + 1) // 2) % 2 if kind == 0 else p // 2)
            partner.append(me + (other - p) * s)
    start = []
    for k in range(COLOURS):
        rows = [0]
        for s in range(6):
            rows.append(rows[-1] + side[(k + s) % 6] * (ROWS >> (s + 1)))
        start.append(rows)

    barrier = pltpu.get_barrier_semaphore()
    for other in partner:
        pl.semaphore_signal(barrier, inc=1, device_id=(rep, other), device_id_type=pl.DeviceIdType.MESH)
    squares_ref[...] = jnp.zeros_like(squares_ref)

    def weights(i):
        layer, at = ((i + PER) // PER) % 2, pl.ds(pl.multiple_of(((i + PER) % PER) * CH, CH), CH)
        slot = (i + PER) % 2
        return [
            pltpu.make_async_copy(wg_ref.at[layer, :, at], w.at[slot, 0], w_sem.at[slot, 0]),
            pltpu.make_async_copy(wu_ref.at[layer, :, at], w.at[slot, 1], w_sem.at[slot, 1]),
            pltpu.make_async_copy(wd_ref.at[layer, at, :], w.at[slot, 2], w_sem.at[slot, 2]),
        ]

    def rows_of(start, size):
        return pl.ds(pl.multiple_of(start, 16), size)

    def exchange(c, stage, k):
        even = c % 2
        if stage < 6:
            size, link = ROWS >> (stage + 1), (k + stage) % 6
            part = pl.ds(place(stage), size)
            source, target = outgoing.at[k, part], incoming.at[even, k, part]
        else:
            s = 11 - stage
            size, link = ROWS >> (s + 1), (k + s) % 6
            source = target = gathered.at[c % GATHERS, k, rows_of(start[k][s + 1], size)]
        return pltpu.make_async_remote_copy(
            src_ref=source,
            dst_ref=target,
            send_sem=sent_sem.at[stage, k],
            recv_sem=got_sem.at[even, stage, k],
            device_id=(rep, partner[link]),
            device_id_type=pl.DeviceIdType.MESH,
        )

    def writes(c):
        layer, first = LAYERS - 1 - c // PER, (c % PER) * CH
        slot, copies = c % GATHERS, []
        for k in range(COLOURS):
            matrix, half = k // 2, (k % 2) * 256
            for b in range(4):
                source = gathered.at[slot, k, pl.ds(b * 256, 256)]
                if matrix < 2:
                    to = (gg_ref, gu_ref)[matrix].at[layer, pl.ds(half, 256), pl.ds(pl.multiple_of(first + b * 128, 128), 128)]
                else:
                    to = gd_ref.at[layer, pl.ds(pl.multiple_of(first + half, 256), 256), pl.ds(b * 128, 128)]
                copies.append(pltpu.make_async_copy(source, to, write_sem.at[k, b]))
        return copies

    def stage_of(stage, c):
        slot, even, gather = c % ACCS, c % 2, c % GATHERS
        if stage == 13:
            for copy in writes(c):
                copy.wait()
            return
        for k in range(COLOURS):
            if stage > 0:
                exchange(c, stage - 1, k).wait()
            if stage < 6:
                size = ROWS >> (stage + 1)
                mine, theirs = side[(k + stage) % 6] * size, (1 - side[(k + stage) % 6]) * size
                goes = acc[slot, k, rows_of(start[k][stage] + theirs, size)]
                if stage > 0:
                    base = place(stage - 1)
                    goes += incoming[even, k, rows_of(base + theirs, size)].astype(jnp.float32)
                    stays = rows_of(start[k][stage] + mine, size)
                    acc[slot, k, stays] += incoming[even, k, rows_of(base + mine, size)].astype(jnp.float32)
                outgoing[k, pl.ds(place(stage), size)] = goes.astype(jnp.bfloat16)
            elif stage == 6:
                rows = rows_of(start[k][6], 16)
                total = acc[slot, k, rows] + incoming[even, k, pl.ds(place(5), 16)].astype(jnp.float32)
                gathered[gather, k, rows] = total.astype(jnp.bfloat16)
            if stage < 12:
                exchange(c, stage, k).start()
        if stage == 12:
            for copy in writes(c):
                copy.start()
            for k in range(COLOURS):
                g = gathered[gather, k].astype(jnp.float32)
                squares_ref[...] += jnp.sum((g * g).reshape(ROWS // 8, 8, 128), axis=0)

    def tile_of(i, phase):
        turn, slot, a_slot = i // PER, i % 2, i % ACCS
        tokens = pl.ds(phase * TILE, TILE)
        a, by = a_ref[turn, tokens, :], ct[turn, tokens, :]
        gate = dot(a, w[slot, 0], NN)
        up = dot(a, w[slot, 1], NN)
        by_p = dot(by, w[slot, 2], NT).astype(jnp.bfloat16).astype(jnp.float32)
        sigmoid = 1 / (1 + jnp.exp(-gate))
        silu = gate * sigmoid
        p = (silu * up).astype(jnp.bfloat16)
        by_up = (by_p * silu).astype(jnp.bfloat16)
        by_gate = (by_p * up * (sigmoid * (1 + gate * (1 - sigmoid)))).astype(jnp.bfloat16)
        for matrix, (l, r) in enumerate(((a, by_gate), (a, by_up), (p, by))):
            g = dot(l, r, TN)
            for half in range(2):
                for b in range(4):
                    part = g[half * 256 : half * 256 + 256, b * 128 : b * 128 + 128]
                    if phase == 0:
                        acc[a_slot, 2 * matrix + half, pl.ds(b * 256, 256)] = part
                    else:
                        acc[a_slot, 2 * matrix + half, pl.ds(b * 256, 256)] += part

        @pl.when(i < PER)
        def _():
            dag[tokens, :] += dot(by_gate, w[slot, 0], NT)
            dau[tokens, :] += dot(by_up, w[slot, 1], NT)

    def next_layer():
        def body(t, _):
            tokens = pl.ds(pl.multiple_of(t * 256, 256), 256)
            d = (dag[tokens, :].astype(jnp.bfloat16).astype(jnp.float32) + dau[tokens, :].astype(jnp.bfloat16).astype(jnp.float32)).astype(jnp.bfloat16)
            d, wide = d.astype(jnp.float32), h_ref[tokens, :].astype(jnp.float32)
            s = scale_of(wide)
            by = d * s - wide * (s * s * s * jnp.sum(d * wide, -1, keepdims=True) * (1 / D))
            ct[1, tokens, :] = (ct[0, tokens, :].astype(jnp.float32) + by.astype(jnp.bfloat16).astype(jnp.float32)).astype(jnp.bfloat16)
            return 0

        lax.fori_loop(0, T // 256, body, 0)

    def first(t, _):
        tokens = pl.ds(pl.multiple_of(t * 256, 256), 256)
        a_ref[1, tokens, :] = normed(h_ref[tokens, :])
        dag[tokens, :] = jnp.zeros((256, D), jnp.float32)
        return 0

    def forward(i, _):
        for copy in weights(i):
            copy.wait()
        for copy in weights(i + 1):
            copy.start()
        slot = (i + PER) % 2

        def tile(t, _):
            tokens = pl.ds(pl.multiple_of(t * TILE, TILE), TILE)
            a = a_ref[1, tokens, :]
            gate = dot(a, w[slot, 0], NN)
            up = dot(a, w[slot, 1], NN)
            p = (gate * (1 / (1 + jnp.exp(-gate))) * up).astype(jnp.bfloat16)
            dag[tokens, :] += dot(p, w[slot, 2], NN)
            return 0

        lax.fori_loop(0, PHASES, tile, 0)
        return 0

    def second(t, _):
        tokens = pl.ds(pl.multiple_of(t * 256, 256), 256)
        h = (h_ref[tokens, :].astype(jnp.float32) + dag[tokens, :].astype(jnp.bfloat16).astype(jnp.float32)).astype(jnp.bfloat16)
        h_ref[tokens, :] = h
        a_ref[0, tokens, :] = normed(h)
        dag[tokens, :] = jnp.zeros((256, D), jnp.float32)
        dau[tokens, :] = jnp.zeros((256, D), jnp.float32)
        return 0

    inputs = [pltpu.make_async_copy(x_ref, h_ref, in_sem.at[0]), pltpu.make_async_copy(dy_ref, ct.at[0], in_sem.at[1])]
    for copy in inputs + weights(-PER):
        copy.start()
    inputs[0].wait()
    lax.fori_loop(0, T // 256, first, 0)
    lax.fori_loop(-PER, 0, forward, 0)
    lax.fori_loop(0, T // 256, second, 0)
    inputs[1].wait()
    pl.semaphore_wait(barrier, 6)

    def body(i, _):
        @pl.when(i < N)
        def _():
            for copy in weights(i):
                copy.wait()

        @pl.when(i + 1 < N)
        def _():
            for copy in weights(i + 1):
                copy.start()

        pl.when(i == PER)(next_layer)

        for phase in range(PHASES):
            pl.when(i < N)(functools.partial(tile_of, i, phase))
            for stage in reversed(range(len(AT))):
                if AT[stage] % PHASES == phase:
                    c = i - AT[stage] // PHASES
                    pl.when((c >= 0) & (c < N))(functools.partial(stage_of, stage, c))
        return 0

    lax.fori_loop(0, N + AT[-1] // PHASES, body, 0)


def gradients_of(x, dy, wg, wu, wd):
    vmem, anywhere = pl.BlockSpec(memory_space=pltpu.VMEM), pl.BlockSpec(memory_space=pl.ANY)
    dma = pltpu.SemaphoreType.DMA
    return pl.pallas_call(
        kernel,
        in_specs=[anywhere] * 5,
        out_specs=[anywhere] * 3 + [vmem],
        out_shape=[
            jax.ShapeDtypeStruct((LAYERS, D, FF), jnp.bfloat16),
            jax.ShapeDtypeStruct((LAYERS, D, FF), jnp.bfloat16),
            jax.ShapeDtypeStruct((LAYERS, FF, D), jnp.bfloat16),
            jax.ShapeDtypeStruct((8, 128), jnp.float32),
        ],
        scratch_shapes=[
            pltpu.VMEM((T, D), jnp.bfloat16),
            pltpu.VMEM((2, T, D), jnp.bfloat16),
            pltpu.VMEM((2, T, D), jnp.bfloat16),
            pltpu.VMEM((T, D), jnp.float32),
            pltpu.VMEM((T, D), jnp.float32),
            pltpu.VMEM((2, 3, D, CH), jnp.bfloat16),
            pltpu.VMEM((ACCS, COLOURS, ROWS, 128), jnp.float32),
            pltpu.VMEM((COLOURS, ROWS, 128), jnp.bfloat16),
            pltpu.VMEM((2, COLOURS, ROWS, 128), jnp.bfloat16),
            pltpu.VMEM((GATHERS, COLOURS, ROWS, 128), jnp.bfloat16),
            dma((2,)),
            dma((2, 3)),
            dma((12, COLOURS)),
            dma((2, 12, COLOURS)),
            dma((COLOURS, 4)),
        ],
        compiler_params=pltpu.CompilerParams(collective_id=0, has_side_effects=True, vmem_limit_bytes=VMEM_LIMIT),
    )(x, dy, wg, wu, wd)


def adamw(w, m, v, g):
    m = 0.9 * m + 0.1 * g
    v = 0.95 * v + 0.05 * g * g
    step = m * lax.rsqrt(v + 1e-8) + 0.1 * w
    return (w - 0.02 * step).astype(jnp.bfloat16), m, v


def solution(mesh):
    def step(x, dy, *arrays):
        weights, m, v = (arrays[i : i + 3] for i in (0, 3, 6))
        *gradients, squares = gradients_of(x[0], dy[0], *weights)
        count = sum(g.size for g in gradients)
        factor = jnp.minimum(1.0, 0.5 * lax.rsqrt(jnp.sum(squares) / count + 1e-30))
        new = [adamw(w.astype(jnp.float32), m, v, g.astype(jnp.float32) * factor) for w, m, v, g in zip(weights, m, v, gradients, strict=True)]
        return tuple(one[which] for which in range(3) for one in new)

    return jax.shard_map(
        step,
        mesh=mesh,
        in_specs=(P(("rep", "dp"), None, None),) * 2 + (P(None, None, None),) * 9,
        out_specs=(P("rep", None, None),) * 9,
        check_vma=False,
    )
```
